32 devices in a mesh: dp: 8 (over z, x), sp: 4 (over y, core).
Axes of the slice: x: 2, y: 2, z: 4, core: 2. Of those that a mesh axis runs over, the one named last changes fastest.
Arguments:
- frames: bfloat16 [8, 1280, 1024], P('dp', 'sp'), may hold values from -6 to 6
- text: bfloat16 [8, 256, 1024], P('dp', 'sp'), may hold values from -6 to 6
- frame_len: int32 [8], P('dp'), may hold values from 1 to 1280, 7680 in all
- text_len: int32 [8], P('dp'), may hold values from 1 to 256, 1024 in all
- cotangent: bfloat16 [8, 1280, 1024], P('dp', 'sp'), may hold values from -6 to 6
- proj_query: bfloat16 [1024, 1024], P('dp'), may hold values from -0.1875 to 0.1875
- proj_key: bfloat16 [1024, 1024], P('dp'), may hold values from -0.1875 to 0.1875
- proj_value: bfloat16 [1024, 1024], P('dp'), may hold values from -0.1875 to 0.1875
- proj_out: bfloat16 [1024, 1024], P('dp'), may hold values from -1.75 to 1.75
- cross_query: bfloat16 [1024, 1024], P('dp'), may hold values from -0.1875 to 0.1875
- cross_key: bfloat16 [1024, 1024], P('dp'), may hold values from -0.1875 to 0.1875
- cross_value: bfloat16 [1024, 1024], P('dp'), may hold values from -0.1875 to 0.1875
- cross_out: bfloat16 [1024, 1024], P('dp'), may hold values from -0.5 to 0.5
- ffn_up: bfloat16 [1024, 4096], P('dp'), may hold values from -0.1875 to 0.1875
- ffn_down: bfloat16 [4096, 1024], P('dp'), may hold values from -0.09375 to 0.09375
- gain_attn: bfloat16 [1024], P('dp'), may hold values from 0.25 to 1.75
- bias_attn: bfloat16 [1024], P('dp'), may hold values from -3 to 3
- gain_cross: bfloat16 [1024], P('dp'), may hold values from 0.25 to 1.75
- bias_cross: bfloat16 [1024], P('dp'), may hold values from -3 to 3
- gain_ffn: bfloat16 [1024], P('dp'), may hold values from 0.25 to 1.75
- bias_ffn: bfloat16 [1024], P('dp'), may hold values from -3 to 3
Outputs:
- output: bfloat16 [8, 1280, 1024], P('dp', 'sp')
- grad_frames: float32 [8, 1280, 1024], P('dp', 'sp')
- grad_text: float32 [8, 256, 1024], P('dp', 'sp')
- grad_proj_query: float32 [1024, 1024], P('dp')
- grad_proj_key: float32 [1024, 1024], P('dp')
- grad_proj_value: float32 [1024, 1024], P('dp')
- grad_proj_out: float32 [1024, 1024], P('dp')
- grad_cross_query: float32 [1024, 1024], P('dp')
- grad_cross_key: float32 [1024, 1024], P('dp')
- grad_cross_value: float32 [1024, 1024], P('dp')
- grad_cross_out: float32 [1024, 1024], P('dp')
- grad_ffn_up: float32 [1024, 4096], P('dp')
- grad_ffn_down: float32 [4096, 1024], P('dp')
- grad_gain_attn: float32 [1024], P('dp')
- grad_bias_attn: float32 [1024], P('dp')
- grad_gain_cross: float32 [1024], P('dp')
- grad_bias_cross: float32 [1024], P('dp')
- grad_gain_ffn: float32 [1024], P('dp')
- grad_bias_ffn: float32 [1024], P('dp')
The draws below stay inside these ranges and needn't reach their ends.
Inputs may be any that keep to these rules, and one draw needn't show every extreme that they name: Each clip's frames 0 to frame_len - 1 are valid; some clip has all 1280 valid. Each clip's text states 0 to text_len - 1 are valid; some clip has all 256 valid.
All inputs are finite; a program needn't handle non-finite values. No bound on the sum of `frame_len` or of `text_len` on one device may be relied on, other than what follows from the above.
Results may differ from the reference program's by a relative error of at most 0.024.
Values may be sent and summed in bfloat16 or wider, within the bound.
A program may use at most 320 MiB of HBM per device.

```python
import math
import jax
import jax.numpy as jnp
import numpy as np
from jax import lax

D = 1024
HEADS = 16
HEAD_DIM = 64
FF = 4096
FRAMES = 1280
TEXT = 256
CLIPS = 8


def spiked(array, key, source, target, shards_of, factor):
    def block_of(position):
        return (jnp.arange(array.shape[position]) // (array.shape[position] // shards_of)).reshape((-1,) + (1,) * (array.ndim - 1 - position))

    one_side = jax.random.permutation(key, shards_of)[block_of(target)]
    far = (block_of(target) + shards_of // 2) % shards_of
    return jnp.where((block_of(source) == one_side) | (block_of(source) == far), factor * array, array)


def level_of(own_key, shape, split, low, largest):
    factor_of, own = 1.0, jax.random.fold_in(own_key, 6)
    for dim, shards_of in split:
        draws = jnp.exp(jax.random.uniform(jax.random.fold_in(own, dim), (shards_of,), jnp.float32, low / len(split), largest / len(split)))
        factor_of = factor_of * jnp.repeat(draws, shape[dim] // shards_of).reshape([-1 if axis == dim else 1 for axis in range(len(shape))])
    return factor_of


def split_up(number_of, total, bound, skew):
    portions = [(1 << 20) // math.isqrt(standing ** skew) + 1 for standing in range(2, number_of + 1)]
    surplus, counts = total - bound - (number_of - 1), [1] * (number_of - 1)
    while surplus > 0:
        movable = [i for i in range(number_of - 1) if counts[i] < bound]
        mass, remaining = sum([portions[i] for i in movable]), surplus
        for i in movable:
            extra = min(bound - counts[i], max(1, remaining * portions[i] // mass), surplus)
            counts[i] = counts[i] + extra
            surplus = surplus - extra
    return np.array([bound] + counts)


def ragged(own_key, number_of, total, most, skew):
    if number_of == 2:
        one = jax.random.randint(own_key, (), max(1, total - most), min(most, total - 1) + 1)
        return jnp.stack([one, total - one])
    tallies = jnp.asarray(split_up(number_of, total, most, skew), jnp.int32)
    twos = (number_of - 1) // 2
    giver, receiver = tallies[1:1 + 2 * twos:2], tallies[2:2 + 2 * twos:2]
    slack = jnp.minimum(giver - 1, most - receiver)
    passed = jax.random.randint(jax.random.fold_in(own_key, 1), (twos,), 0, 1 << 20) % (slack + 1)
    tallies = tallies.at[1:1 + 2 * twos:2].set(giver - passed).at[2:2 + 2 * twos:2].set(receiver + passed)
    return tallies[jax.random.permutation(jax.random.fold_in(own_key, 2), number_of)]


def gaussian(stream_key, extent, deviation, limit, cuts=(), kind=jnp.bfloat16):
    values = jax.random.normal(stream_key, extent, jnp.float32) * deviation
    if len(cuts) > 0:
        values = level_of(stream_key, extent, cuts, -0.22, 0.18) * values
    return jnp.clip(values, min=-limit, max=limit).astype(kind)


def noise_with(key, dims, deviation, most, cuts, heavy, kind=jnp.bfloat16):
    array = deviation * jax.random.normal(key, dims, jnp.float32)
    if cuts:
        array = array * level_of(key, dims, cuts, -0.22, 0.18)
    return jnp.clip(spiked(array, jax.random.fold_in(key, 3), *heavy), -most, most).astype(kind)


def setup_inputs(seed: int = 0) -> dict:
    seeds = jax.random.split(jax.random.key(seed), 22)
    frames = noise_with(seeds[0], (CLIPS, FRAMES, D), 1.0, 6.0, ((0, 8), (1, 4)), (0, 2, 8, 2.0))
    text = gaussian(seeds[1], (CLIPS, TEXT, D), 1.0, 6.0, ((0, 8), (1, 4)))
    frame_len = ragged(seeds[2], CLIPS, CLIPS * FRAMES * 3 // 4, FRAMES, 1).astype(jnp.int32)
    text_len = ragged(seeds[3], CLIPS, CLIPS * TEXT // 2, TEXT, 1).astype(jnp.int32)
    cotangent = gaussian(seeds[4], (CLIPS, FRAMES, D), 1.0, 6.0, ((0, 8), (1, 4)))
    proj_query = gaussian(seeds[5], (D, D), D ** -0.5, 0.1875, ((0, 8),))
    proj_key = gaussian(seeds[6], (D, D), D ** -0.5, 0.1875, ((0, 8),))
    proj_value = gaussian(seeds[7], (D, D), D ** -0.5, 0.1875, ((0, 8),))
    proj_out = gaussian(seeds[8], (D, D), (D * 16 // FRAMES) ** -0.5, 1.75, ((0, 8),))
    cross_query = gaussian(seeds[9], (D, D), D ** -0.5, 0.1875, ((0, 8),))
    cross_key = gaussian(seeds[10], (D, D), D ** -0.5, 0.1875, ((0, 8),))
    cross_value = gaussian(seeds[11], (D, D), D ** -0.5, 0.1875, ((0, 8),))
    cross_out = gaussian(seeds[12], (D, D), (D * 32 // TEXT) ** -0.5, 0.5, ((0, 8),))
    ffn_up = gaussian(seeds[13], (D, FF), D ** -0.5, 0.1875, ((0, 8),))
    ffn_down = gaussian(seeds[14], (FF, D), FF ** -0.5, 0.09375, ((0, 8),))
    gain_attn = jnp.clip(1.0 + 0.15 * jax.random.normal(seeds[15], (D,), jnp.float32), 0.25, 1.75).astype(jnp.bfloat16)
    bias_attn = gaussian(seeds[16], (D,), 0.5, 3.0, ((0, 8),))
    gain_cross = jnp.clip(1.0 + 0.15 * jax.random.normal(seeds[17], (D,), jnp.float32), 0.25, 1.75).astype(jnp.bfloat16)
    bias_cross = gaussian(seeds[18], (D,), 0.5, 3.0, ((0, 8),))
    gain_ffn = jnp.clip(1.0 + 0.15 * jax.random.normal(seeds[19], (D,), jnp.float32), 0.25, 1.75).astype(jnp.bfloat16)
    bias_ffn = gaussian(seeds[20], (D,), 0.5, 3.0, ((0, 8),))
    return {"frames": frames, "text": text, "frame_len": frame_len, "text_len": text_len, "cotangent": cotangent, "proj_query": proj_query, "proj_key": proj_key, "proj_value": proj_value, "proj_out": proj_out, "cross_query": cross_query, "cross_key": cross_key, "cross_value": cross_value, "cross_out": cross_out, "ffn_up": ffn_up, "ffn_down": ffn_down, "gain_attn": gain_attn, "bias_attn": bias_attn, "gain_cross": gain_cross, "bias_cross": bias_cross, "gain_ffn": gain_ffn, "bias_ffn": bias_ffn}


@jax.custom_vjp
def low(v):
    return lax.optimization_barrier(v.astype(jnp.bfloat16)).astype(jnp.float32)

@jax.custom_vjp
def low_back(v):
    return v

def low_keep(v):
    return (low(v), None)

def low_pass(kept, grad):
    return (grad,)

def back_keep(v):
    return (v, None)

def back_low(kept, grad):
    return (low(grad),)
low.defvjp(low_keep, low_pass)
low_back.defvjp(back_keep, back_low)
epsilon = 1e-05
negative = -1e+30

def both_ways(values):
    return low(low_back(values))

def layer_norm(values, gain_vec, offset):
    centre = lax.optimization_barrier(jnp.mean(values, axis=-1, keepdims=True))
    spread = lax.optimization_barrier(jnp.mean(jnp.square(values - centre), axis=-1, keepdims=True))
    return (values - centre) * lax.rsqrt(spread + epsilon) * gain_vec + offset

def mat_mul(first_op, second_op):
    return jnp.dot(first_op, second_op, precision=lax.Precision.HIGHEST)

def attention(queries, key_rows, values, visible):
    n_rows = queries.shape[0]
    n_keys = key_rows.shape[0]
    factor = HEAD_DIM ** (-0.5)
    q_heads = queries.reshape(n_rows, HEADS, HEAD_DIM)
    k_heads = key_rows.reshape(n_keys, HEADS, HEAD_DIM)
    v_heads = values.reshape(n_keys, HEADS, HEAD_DIM)
    score = low_back(factor * jnp.einsum('qhd,khd->hqk', q_heads, k_heads, precision=lax.Precision.HIGHEST))
    score = jnp.where(visible[None], score, negative)
    row_max = lax.optimization_barrier(jnp.max(score, axis=2, keepdims=True))
    raised = jnp.exp(score - row_max)
    probs = raised / lax.optimization_barrier(jnp.sum(raised, axis=2, keepdims=True))
    mixed = jnp.einsum('hqk,khd->qhd', low(probs), v_heads, precision=lax.Precision.HIGHEST)
    return both_ways(mixed.reshape(n_rows, HEADS * HEAD_DIM))

def layer_clip(params, item):
    frames, text, frame_count, text_count = item
    proj_query, proj_key, proj_value, proj_out, cross_query, cross_key, cross_value, cross_out, ffn_up, ffn_down, gain_attn, bias_attn, gain_cross, bias_cross, gain_ffn, bias_ffn = params
    n_rows = frames.shape[0]
    n_text = text.shape[0]
    positions = jnp.arange(n_rows, dtype=jnp.int32)
    text_pos = jnp.arange(n_text, dtype=jnp.int32)
    causal = (positions[None, :] < frame_count) & (positions[None, :] <= positions[:, None])
    reach = jnp.broadcast_to(text_pos[None, :] < text_count, (n_rows, n_text))
    normed1 = low(layer_norm(frames, gain_attn, bias_attn))
    context = attention(both_ways(mat_mul(normed1, proj_query)), both_ways(mat_mul(normed1, proj_key)), both_ways(mat_mul(normed1, proj_value)), causal)
    middle = frames + low_back(mat_mul(context, proj_out))
    normed2 = low(layer_norm(middle, gain_cross, bias_cross))
    context2 = attention(both_ways(mat_mul(normed2, cross_query)), both_ways(mat_mul(text, cross_key)), both_ways(mat_mul(text, cross_value)), reach)
    after = middle + low_back(mat_mul(context2, cross_out))
    normed3 = low(layer_norm(after, gain_ffn, bias_ffn))
    hidden = low(jax.nn.gelu(low_back(mat_mul(normed3, ffn_up)), approximate=False))
    return after + low_back(mat_mul(hidden, ffn_down))

def reference(frames, text, frame_len, text_len, cotangent, proj_query, proj_key, proj_value, proj_out, cross_query, cross_key, cross_value, cross_out, ffn_up, ffn_down, gain_attn, bias_attn, gain_cross, bias_cross, gain_ffn, bias_ffn):
    params = tuple((weight.astype(jnp.float32) for weight in (proj_query, proj_key, proj_value, proj_out, cross_query, cross_key, cross_value, cross_out, ffn_up, ffn_down, gain_attn, bias_attn, gain_cross, bias_cross, gain_ffn, bias_ffn)))

    def forward(frames_wide, text_wide, params_wide):

        def clip_step(item):
            return layer_clip(params_wide, item)
        return lax.map(jax.checkpoint(clip_step), (frames_wide, text_wide, frame_len, text_len))
    result, pull = jax.vjp(forward, frames.astype(jnp.float32), text.astype(jnp.float32), params)
    grad_frames, grad_text, grads = pull(cotangent.astype(jnp.float32))
    return (result.astype(jnp.bfloat16), grad_frames, grad_text, grads[0], grads[1], grads[2], grads[3], grads[4], grads[5], grads[6], grads[7], grads[8], grads[9], grads[10], grads[11], grads[12], grads[13], grads[14], grads[15])
```

```python
from functools import partial

import jax
import jax.numpy as jnp
from jax import lax
from jax.sharding import PartitionSpec as P

HEAD_DIM = 64
EPS = 1e-05
NEGATIVE = -1e30
BF = jnp.bfloat16
F32 = jnp.float32


def mm(a, b):
    return jnp.dot(a, b, preferred_element_type=F32)


def mm_t(a, b):
    return lax.dot_general(a, b, (((1,), (1,)), ((), ())), preferred_element_type=F32)


def t_mm(a, b):
    return lax.dot_general(a, b, (((0,), (0,)), ((), ())), preferred_element_type=F32)


def norm_parts(rows):
    centre = jnp.mean(rows, axis=-1, keepdims=True)
    spread = jnp.mean(jnp.square(rows - centre), axis=-1, keepdims=True)
    inv = lax.rsqrt(spread + EPS)
    return (rows - centre) * inv, inv


def norm_back(grad, xhat, inv, gain):
    scaled = grad * gain
    return inv * (
        scaled
        - jnp.mean(scaled, axis=-1, keepdims=True)
        - xhat * jnp.mean(scaled * xhat, axis=-1, keepdims=True)
    )


def visible_of(n_rows, n_keys, length, causal):
    cols = lax.broadcasted_iota(jnp.int32, (n_rows, n_keys), 1)
    seen = cols < length
    if causal:
        seen = seen & (cols <= lax.broadcasted_iota(jnp.int32, (n_rows, n_keys), 0))
    return seen


def attend(q, k, v, length, causal):
    factor = HEAD_DIM ** (-0.5)
    seen = visible_of(q.shape[0], k.shape[0], length, causal)
    outs, sums = [], []
    for at in range(0, q.shape[1], HEAD_DIM):
        cols = slice(at, at + HEAD_DIM)
        score = jnp.where(seen, mm_t(q[:, cols], k[:, cols]) * factor, NEGATIVE)
        top = jnp.max(score, axis=1, keepdims=True)
        raised = jnp.exp(score - top)
        total = jnp.sum(raised, axis=1, keepdims=True)
        outs.append(mm((raised / total).astype(BF), v[:, cols]))
        sums.append(top + jnp.log(total))
    return jnp.concatenate(outs, axis=1).astype(BF), jnp.concatenate(sums, axis=1)


def attend_back(q, k, v, dctx, lse, length, causal):
    factor = HEAD_DIM ** (-0.5)
    seen = visible_of(q.shape[0], k.shape[0], length, causal)
    dqs, dks, dvs = [], [], []
    for head, at in enumerate(range(0, q.shape[1], HEAD_DIM)):
        cols = slice(at, at + HEAD_DIM)
        score = mm_t(q[:, cols], k[:, cols]) * factor
        probs = jnp.where(seen, jnp.exp(score - lse[:, head : head + 1]), 0.0)
        dprobs = mm_t(dctx[:, cols], v[:, cols])
        inner = jnp.sum(probs * dprobs, axis=1, keepdims=True)
        dscore = (probs * (dprobs - inner)).astype(BF)
        dqs.append(mm(dscore, k[:, cols]) * factor)
        dks.append(t_mm(dscore, q[:, cols]) * factor)
        dvs.append(t_mm(probs.astype(BF), dctx[:, cols]))
    return tuple(jnp.concatenate(part, axis=1).astype(BF) for part in (dqs, dks, dvs))


def gather_rows(block):
    return lax.all_gather(block, "sp", axis=0, tiled=True)


def gather_cols(block):
    return lax.all_gather(block, "sp", axis=1, tiled=True)


def scatter_rows(part):
    return lax.psum_scatter(part.astype(BF), "sp", scatter_dimension=0, tiled=True).astype(F32)


def gelu_parts(u):
    phi = 0.5 * (1.0 + lax.erf(u * (2.0**-0.5)))
    slope = phi + u * jnp.exp(-0.5 * u * u) * ((2.0 * jnp.pi) ** -0.5)
    return u * phi, slope


def on_device(n_dp, n_sp, *arrays):
    (
        frames, text, frame_len, text_len, cotangent,
        w_q, w_k, w_v, w_o, c_q, c_k, c_v, c_o, f_up, f_down,
        gain_a, bias_a, gain_c, bias_c, gain_f, bias_f,
    ) = arrays
    clips, local, width = frames.shape
    assert clips == 1
    rank = lax.axis_index("sp")
    own = width // n_sp
    block = w_q.shape[0]
    hidden = f_up.shape[1]
    unit = f_down.shape[0] // n_sp
    flen, tlen = frame_len[0], text_len[0]

    def own_cols(weight):
        return lax.dynamic_slice_in_dim(weight, rank * own, own, axis=1)

    def own_rows(rows):
        return lax.dynamic_slice_in_dim(rows, rank * local, local, axis=0)

    def from_dp(part):
        return lax.all_gather(part, "dp", axis=0, tiled=True)

    small = jnp.stack([gain_a, bias_a, gain_c, bias_c, gain_f, bias_f], axis=1)
    small = jnp.pad(small, ((0, 0), (0, 128 - small.shape[1])))
    first = from_dp(jnp.concatenate([own_cols(w) for w in (w_q, w_k, w_v)] + [small], axis=1))
    second = from_dp(jnp.concatenate([own_cols(w) for w in (w_o, c_q, c_o, c_k, c_v)], axis=1))
    up_own = lax.dynamic_slice_in_dim(
        f_up.reshape(block, n_dp, n_sp, unit), rank, 1, axis=2
    ).reshape(block, n_dp * unit)
    up = from_dp(up_own)
    down = from_dp(lax.dynamic_slice_in_dim(f_down, rank * unit, unit, axis=0))

    qkv_w = first[:, : 3 * own]
    vecs = first[:, 3 * own : 3 * own + 6].astype(F32).T
    ga, ba, gc, bc, gf, bf = (vecs[i : i + 1] for i in range(6))
    full3 = lax.all_gather(second[:, : 3 * own], "sp", axis=0, tiled=False)
    o_full, cq_full, co_full = (
        jnp.transpose(full3[:, :, i * own : (i + 1) * own], (1, 0, 2)).reshape(width, width)
        for i in range(3)
    )
    cq_own = second[:, own : 2 * own]
    ckv_own = second[:, 3 * own :]

    x = gather_rows(frames[0]).astype(F32)
    cot = gather_rows(cotangent[0])
    txt = gather_rows(text[0])

    hat1, _ = norm_parts(x)
    h1 = (hat1 * ga + ba).astype(BF)
    qkv = mm(h1, qkv_w).astype(BF)
    q, k, v = (qkv[:, i * own : (i + 1) * own] for i in range(3))
    ctx_own, lse = attend(q, k, v, flen, True)
    ctx = gather_cols(ctx_own)
    mid = x + mm(ctx, o_full)
    hat2, inv2 = norm_parts(mid)
    h2 = (hat2 * gc + bc).astype(BF)
    q2 = mm(h2, cq_own).astype(BF)
    kv2 = mm(txt, ckv_own).astype(BF)
    k2, v2 = kv2[:, :own], kv2[:, own:]
    ctx2_own, lse2 = attend(q2, k2, v2, tlen, False)
    ctx2 = gather_cols(ctx2_own)
    after = mid + mm(ctx2, co_full)
    hat3, _ = norm_parts(after)
    h3 = (hat3 * gf + bf).astype(BF)
    u = mm(h3, up)
    act, slope = gelu_parts(u)
    act = act.astype(BF)
    after_own = own_rows(after)
    output = (after_own + scatter_rows(mm(act, down))).astype(BF).reshape(frames.shape)

    du = (mm_t(cot, down) * slope).astype(BF)
    part_down = t_mm(act, cot).astype(BF).reshape(n_dp * block, unit * width // block)
    part_ffn = jnp.concatenate([part_down, t_mm(h3, du).astype(BF)], axis=1)
    sum_ffn = lax.psum_scatter(part_ffn, "dp", scatter_dimension=0, tiled=True)
    e3 = scatter_rows(mm_t(du, up))
    hat, inv = norm_parts(after_own)
    d_after_own = cotangent[0].astype(F32) + norm_back(e3, hat, inv, gf)
    sums = [jnp.sum(e3 * hat, axis=0), jnp.sum(e3, axis=0)]
    da2 = gather_rows(d_after_own.astype(BF))
    dctx2 = mm_t(da2, lax.dynamic_slice_in_dim(co_full, rank * own, own, axis=0)).astype(BF)
    dq2, dk2, dv2 = attend_back(q2, k2, v2, dctx2, lse2, tlen, False)
    dq2_full = gather_cols(dq2)
    part_cross = jnp.concatenate(
        [t_mm(ctx2, own_cols(da2)), t_mm(h2, dq2), t_mm(txt, jnp.concatenate([dk2, dv2], axis=1))],
        axis=1,
    ).astype(BF)
    sum_cross = lax.psum_scatter(part_cross, "dp", scatter_dimension=0, tiled=True)
    grad_text = scatter_rows(mm_t(jnp.concatenate([dk2, dv2], axis=1), ckv_own))
    e2 = mm_t(dq2_full, cq_full)
    back2 = norm_back(e2, hat2, inv2, gc)
    da = (da2.astype(F32) + back2).astype(BF)
    e2_own = own_rows(e2)
    hat2_own = own_rows(hat2)
    d_mid_own = d_after_own + own_rows(back2)
    sums = [jnp.sum(e2_own * hat2_own, axis=0), jnp.sum(e2_own, axis=0)] + sums
    dctx = mm_t(da, lax.dynamic_slice_in_dim(o_full, rank * own, own, axis=0)).astype(BF)
    dq, dk, dv = attend_back(q, k, v, dctx, lse, flen, True)
    dqkv = jnp.concatenate([dq, dk, dv], axis=1)
    e1 = scatter_rows(mm_t(dqkv, qkv_w))
    hat, inv = norm_parts(frames[0].astype(F32))
    grad_frames = (d_mid_own + norm_back(e1, hat, inv, ga)).reshape(frames.shape)
    sums = [jnp.sum(e1 * hat, axis=0), jnp.sum(e1, axis=0)] + sums
    sums = jnp.pad(jnp.stack(sums, axis=1), ((0, 0), (0, 122)))
    part_self = jnp.concatenate(
        [t_mm(ctx, own_cols(da)), t_mm(h1, dqkv), sums], axis=1
    ).astype(BF)
    sum_self = lax.psum_scatter(part_self, "dp", scatter_dimension=0, tiled=True)

    done = lax.all_gather(
        jnp.concatenate([sum_ffn, sum_cross, sum_self], axis=1), "sp", axis=0, tiled=False
    ).astype(F32)
    at = unit * width // block
    grad_down = done[:, :, :at].reshape(n_sp * unit, width)
    grad_up = done[:, :, at : at + n_dp * unit].reshape(n_sp, block, n_dp, unit)
    grad_up = jnp.transpose(grad_up, (1, 2, 0, 3)).reshape(block, hidden)
    at += n_dp * unit
    squares = []
    for _ in range(8):
        squares.append(jnp.transpose(done[:, :, at : at + own], (1, 0, 2)).reshape(block, width))
        at += own
    g_co, g_cq, g_ck, g_cv, g_o, g_q, g_k, g_v = squares
    vec = jnp.sum(done[:, :, at : at + 6], axis=0)
    return (
        output, grad_frames, grad_text.reshape(text.shape),
        g_q, g_k, g_v, g_o, g_cq, g_ck, g_cv, g_co, grad_up, grad_down,
    ) + tuple(vec[:, i] for i in range(6))


def solution(mesh):
    rows, flat, vec = P("dp", "sp", None), P("dp", None), P("dp")
    return jax.shard_map(
        partial(on_device, mesh.shape["dp"], mesh.shape["sp"]),
        mesh=mesh,
        in_specs=(rows, rows, vec, vec, rows) + (flat,) * 10 + (vec,) * 6,
        out_specs=(rows, rows, rows) + (flat,) * 10 + (vec,) * 6,
        check_vma=False,
    )
```

```python
from functools import partial

import jax
import jax.numpy as jnp
from jax import lax
from jax.experimental import pallas as pl
from jax.experimental.pallas import tpu as pltpu
from jax.sharding import PartitionSpec as P

HEAD_DIM = 64
EPS = 1e-05
NEGATIVE = -1e30
BF = jnp.bfloat16
F32 = jnp.float32


def mm(a, b):
    return jnp.dot(a, b, preferred_element_type=F32)


def mm_t(a, b):
    return lax.dot_general(a, b, (((1,), (1,)), ((), ())), preferred_element_type=F32)


def t_mm(a, b):
    return lax.dot_general(a, b, (((0,), (0,)), ((), ())), preferred_element_type=F32)


def norm_parts(rows):
    centre = jnp.mean(rows, axis=-1, keepdims=True)
    spread = jnp.mean(jnp.square(rows - centre), axis=-1, keepdims=True)
    inv = lax.rsqrt(spread + EPS)
    return (rows - centre) * inv, inv


def norm_back(grad, xhat, inv, gain):
    scaled = grad * gain
    return inv * (
        scaled
        - jnp.mean(scaled, axis=-1, keepdims=True)
        - xhat * jnp.mean(scaled * xhat, axis=-1, keepdims=True)
    )


def dot_nt(a, b):
    return lax.dot_general(a, b, (((1,), (1,)), ((), ())), preferred_element_type=F32)


def key_bias(length, n_keys, n_queries, causal):
    rows = lax.broadcasted_iota(jnp.int32, (n_keys, 1), 0)
    bias = jnp.where(rows < length, 0.0, NEGATIVE)
    if not causal:
        return bias, None
    key = lax.broadcasted_iota(jnp.int32, (n_queries, n_queries), 0)
    query = lax.broadcasted_iota(jnp.int32, (n_queries, n_queries), 1)
    return bias, jnp.where(key <= query, 0.0, NEGATIVE)


def scores_t(keys, queries, bias, corner):
    scores = dot_nt(keys, queries)
    if corner is None:
        return scores + bias
    n = corner.shape[0]
    low = scores[-n:] + (bias[-n:] + corner)
    if keys.shape[0] == n:
        return low
    return jnp.concatenate([scores[:-n] + bias[:-n], low], axis=0)


def attend_kernel(causal, step, length_ref, q_ref, k_ref, v_ref, ctx_ref, lse_ref, vt, ctxt):
    heads = q_ref.shape[1] // HEAD_DIM
    n_rows, n_keys = q_ref.shape[0], k_ref.shape[0]
    vt[...] = v_ref[...].T
    lane = lax.broadcasted_iota(jnp.int32, (1, q_ref.shape[1]), 1) // HEAD_DIM
    bias, corner = key_bias(length_ref[0], n_keys, step, causal)

    def one_head(head, carry):
        mask = jnp.where(lane == head, HEAD_DIM**-0.5, 0.0).astype(BF)
        dims = pl.ds(pl.multiple_of(head * HEAD_DIM, HEAD_DIM), HEAD_DIM)
        for at in range(0, n_rows, step):
            seen = at + step if causal else n_keys
            queries = q_ref[at : at + step, :] * mask
            scores = scores_t(k_ref[:seen, :], queries, bias[:seen], corner)
            top = jnp.max(scores, axis=0, keepdims=True)
            raised = jnp.exp(scores - top)
            total = jnp.sum(raised, axis=0, keepdims=True)
            mixed = jnp.dot(vt[dims, :seen], raised.astype(BF), preferred_element_type=F32)
            ctxt[dims, at : at + step] = mixed / total
            lse_ref[pl.ds(head, 1), at : at + step] = top + jnp.log(total)
        return carry

    lax.fori_loop(0, heads, one_head, 0)
    ctx_ref[...] = ctxt[...].T.astype(BF)


def attend_back_kernel(
    causal, step, length_ref, q_ref, k_ref, v_ref, d_ref, lse_ref, dq_ref, dk_ref, dv_ref,
    kt, dqt, dk_sum, dv_sum,
):
    heads = q_ref.shape[1] // HEAD_DIM
    n_rows, n_keys = q_ref.shape[0], k_ref.shape[0]
    kt[...] = k_ref[...].T
    dk_sum[...] = jnp.zeros_like(dk_sum)
    dv_sum[...] = jnp.zeros_like(dv_sum)
    lane = lax.broadcasted_iota(jnp.int32, (1, q_ref.shape[1]), 1) // HEAD_DIM
    bias, corner = key_bias(length_ref[0], n_keys, step, causal)

    def one_head(head, carry):
        mask = jnp.where(lane == head, HEAD_DIM**-0.5, 0.0).astype(BF)
        plain = jnp.where(lane == head, 1.0, 0.0).astype(BF)
        dims = pl.ds(pl.multiple_of(head * HEAD_DIM, HEAD_DIM), HEAD_DIM)
        for at in range(0, n_rows, step):
            seen = at + step if causal else n_keys
            queries = q_ref[at : at + step, :] * mask
            grads = d_ref[at : at + step, :] * plain
            scores = scores_t(k_ref[:seen, :], queries, bias[:seen], corner)
            probs = jnp.exp(scores - lse_ref[pl.ds(head, 1), at : at + step])
            dprobs = dot_nt(v_ref[:seen, :], grads)
            inner = jnp.sum(probs * dprobs, axis=0, keepdims=True)
            dscores = (probs * (dprobs - inner)).astype(BF)
            dqt[dims, at : at + step] = jnp.dot(
                kt[dims, :seen], dscores, preferred_element_type=F32
            ) * (HEAD_DIM**-0.5)
            dk_sum[:seen, :] += jnp.dot(dscores, queries, preferred_element_type=F32)
            dv_sum[:seen, :] += jnp.dot(probs.astype(BF), grads, preferred_element_type=F32)
        return carry

    lax.fori_loop(0, heads, one_head, 0)
    dq_ref[...] = dqt[...].T.astype(BF)
    dk_ref[...] = dk_sum[...].astype(BF)
    dv_ref[...] = dv_sum[...].astype(BF)


STEP = 256
VMEM = pl.BlockSpec(memory_space=pltpu.VMEM)
SMEM = pl.BlockSpec(memory_space=pltpu.SMEM)
LIMIT = 60 * 2**20


def lse_rows(q):
    return max(8, q.shape[1] // HEAD_DIM)


def attend(q, k, v, length, causal):
    n_rows, own = q.shape
    n_keys = k.shape[0]
    work = n_rows * n_keys * own
    return pl.pallas_call(
        partial(attend_kernel, causal, STEP),
        out_shape=(
            jax.ShapeDtypeStruct((n_rows, own), BF),
            jax.ShapeDtypeStruct((lse_rows(q), n_rows), F32),
        ),
        in_specs=[SMEM, VMEM, VMEM, VMEM],
        out_specs=(VMEM, VMEM),
        scratch_shapes=[pltpu.VMEM((own, n_keys), BF), pltpu.VMEM((own, n_rows), F32)],
        compiler_params=pltpu.CompilerParams(vmem_limit_bytes=LIMIT),
        cost_estimate=pl.CostEstimate(
            flops=8 * work, bytes_accessed=4 * q.size * 2, transcendentals=work // HEAD_DIM
        ),
        name="attend",
    )(length, q, k, v)


def attend_back(q, k, v, dctx, lse, length, causal):
    n_rows, own = q.shape
    n_keys = k.shape[0]
    work = n_rows * n_keys * own
    return pl.pallas_call(
        partial(attend_back_kernel, causal, STEP),
        out_shape=(
            jax.ShapeDtypeStruct((n_rows, own), BF),
            jax.ShapeDtypeStruct((n_keys, own), BF),
            jax.ShapeDtypeStruct((n_keys, own), BF),
        ),
        in_specs=[SMEM] + [VMEM] * 5,
        out_specs=(VMEM, VMEM, VMEM),
        scratch_shapes=[
            pltpu.VMEM((own, n_keys), BF),
            pltpu.VMEM((own, n_rows), F32),
            pltpu.VMEM((n_keys, own), F32),
            pltpu.VMEM((n_keys, own), F32),
        ],
        compiler_params=pltpu.CompilerParams(vmem_limit_bytes=LIMIT),
        cost_estimate=pl.CostEstimate(
            flops=20 * work, bytes_accessed=7 * q.size * 2, transcendentals=work // HEAD_DIM
        ),
        name="attend_back",
    )(length, q, k, v, dctx, lse)


def sp_place(n_sp):
    me = lax.axis_index("sp")
    side = lax.rem(me, 2)
    return me, me // 2, side, me + 1 - 2 * side, n_sp // 2


def sp_barrier(n_sp):
    me, y, side, partner, n_y = sp_place(n_sp)
    barrier = pltpu.get_barrier_semaphore()
    pl.semaphore_signal(barrier, inc=1, device_id={"sp": partner})
    for far in range(1, n_y):
        peer = lax.rem(y + far, n_y) * 2 + side
        pl.semaphore_signal(barrier, inc=1, device_id={"sp": peer})
    pl.semaphore_wait(barrier, n_y)


def remote(src, dst, send, recv, peer):
    return pltpu.make_async_remote_copy(
        src_ref=src, dst_ref=dst, send_sem=send, recv_sem=recv, device_id={"sp": peer}
    )


def gather_kernel(n_sp, axes, *refs):
    count = len(axes)
    ins, outs = refs[:count], refs[count : 2 * count]
    send, recv = refs[2 * count :]
    me, y, side, partner, n_y = sp_place(n_sp)

    def spot(which, owner):
        size = ins[which].shape[axes[which]]
        span = pl.ds(pl.multiple_of(owner * size, size), size)
        return outs[which].at[span] if axes[which] == 0 else outs[which].at[:, span]

    sp_barrier(n_sp)
    copies = []
    for which in range(count):
        for far in range(1, n_y):
            peer = lax.rem(y + far, n_y) * 2 + side
            copies.append(
                remote(ins[which], spot(which, me), send.at[which, far], recv.at[which, far], peer)
            )
            copies[-1].start()
        copies.append(
            remote(ins[which], spot(which, me), send.at[which, 0], recv.at[which, 0], partner)
        )
        copies[-1].start()
    for which in range(count):
        spot(which, me)[...] = ins[which][...]
    relays = []
    for which in range(count):
        for far in range(1, n_y):
            copies[which * n_y + far - 1].wait_recv()
            origin = lax.rem(y + n_y - far, n_y) * 2 + side
            at = spot(which, origin)
            slot = n_y - 1 + far
            relays.append(remote(at, at, send.at[which, slot], recv.at[which, slot], partner))
            relays[-1].start()
    for which in range(count):
        for far in range(1, n_y):
            copies[which * n_y + far - 1].wait_send()
        copies[which * n_y + n_y - 1].wait()
    for copy in relays:
        copy.wait()


def sp_gather(n_sp, ident, blocks, axes):
    shapes = []
    for block, axis in zip(blocks, axes):
        shape = list(block.shape)
        shape[axis] *= n_sp
        shapes.append(jax.ShapeDtypeStruct(tuple(shape), block.dtype))
    sent = sum(block.size * block.dtype.itemsize for block in blocks) * n_sp
    return pl.pallas_call(
        partial(gather_kernel, n_sp, axes),
        out_shape=tuple(shapes),
        in_specs=[VMEM] * len(blocks),
        out_specs=(VMEM,) * len(blocks),
        scratch_shapes=[
            pltpu.SemaphoreType.DMA((len(blocks), n_sp)),
            pltpu.SemaphoreType.DMA((len(blocks), n_sp)),
        ],
        compiler_params=pltpu.CompilerParams(
            collective_id=ident, has_side_effects=True, vmem_limit_bytes=LIMIT
        ),
        cost_estimate=pl.CostEstimate(flops=0, bytes_accessed=20 * sent, transcendentals=0),
        name="sp_gather",
    )(*blocks)


def scatter_kernel(n_sp, part_ref, out_ref, near, chip, far_in, send, recv):
    me, y, side, partner, n_y = sp_place(n_sp)
    size = out_ref.shape[0]

    def mine(owner):
        return part_ref.at[pl.ds(pl.multiple_of(owner * size, size), size)]

    sp_barrier(n_sp)
    firsts, seconds = [], []
    for far in range(1, n_y + 1):
        row = lax.rem(y + far, n_y)
        slot = far % n_y
        firsts.append(
            remote(mine(row * 2 + 1 - side), near.at[slot], send.at[slot], recv.at[slot], partner)
        )
        firsts[-1].start()
    for far in range(1, n_y):
        peer = lax.rem(y + far, n_y) * 2 + side
        firsts[far - 1].wait_recv()
        chip[far] = (mine(peer)[...].astype(F32) + near[far].astype(F32)).astype(BF)
        slot = n_y - 1 + far
        seconds.append(remote(chip.at[far], far_in.at[far], send.at[slot], recv.at[slot], peer))
        seconds[-1].start()
    firsts[n_y - 1].wait_recv()
    out_ref[...] = mine(me)[...].astype(F32) + near[0].astype(F32)
    for far in range(1, n_y):
        seconds[far - 1].wait_recv()
        out_ref[...] += far_in[far].astype(F32)
    for copy in firsts + seconds:
        copy.wait_send()


def sp_scatter(n_sp, ident, part):
    rows, width = part.shape
    size, n_y = rows // n_sp, n_sp // 2
    room = pltpu.VMEM((n_y, size, width), BF)
    return pl.pallas_call(
        partial(scatter_kernel, n_sp),
        out_shape=jax.ShapeDtypeStruct((size, width), F32),
        in_specs=[VMEM],
        out_specs=VMEM,
        scratch_shapes=[room, room, room]
        + [pltpu.SemaphoreType.DMA((n_sp,)), pltpu.SemaphoreType.DMA((n_sp,))],
        compiler_params=pltpu.CompilerParams(
            collective_id=ident, has_side_effects=True, vmem_limit_bytes=LIMIT
        ),
        cost_estimate=pl.CostEstimate(flops=0, bytes_accessed=40 * part.size, transcendentals=0),
        name="sp_scatter",
    )(part.astype(BF))


def gelu_parts(u):
    phi = 0.5 * (1.0 + lax.erf(u * (2.0**-0.5)))
    slope = phi + u * jnp.exp(-0.5 * u * u) * ((2.0 * jnp.pi) ** -0.5)
    return u * phi, slope


def on_device(n_dp, n_sp, *arrays):
    (
        frames, text, frame_len, text_len, cotangent,
        w_q, w_k, w_v, w_o, c_q, c_k, c_v, c_o, f_up, f_down,
        gain_a, bias_a, gain_c, bias_c, gain_f, bias_f,
    ) = arrays
    clips, local, width = frames.shape
    assert clips == 1
    rank = lax.axis_index("sp")
    own = width // n_sp
    block = w_q.shape[0]
    hidden = f_up.shape[1]
    unit = f_down.shape[0] // n_sp
    flen, tlen = frame_len, text_len

    def own_cols(weight):
        return lax.dynamic_slice_in_dim(weight, rank * own, own, axis=1)

    def own_rows(rows):
        return lax.dynamic_slice_in_dim(rows, rank * local, local, axis=0)

    def from_dp(part):
        return lax.all_gather(part, "dp", axis=0, tiled=True)

    small = jnp.stack([gain_a, bias_a, gain_c, bias_c, gain_f, bias_f], axis=1)
    small = jnp.pad(small, ((0, 0), (0, 128 - small.shape[1])))
    first = from_dp(jnp.concatenate([own_cols(w) for w in (w_q, w_k, w_v)] + [small], axis=1))
    second = from_dp(jnp.concatenate([own_cols(w) for w in (w_o, c_q, c_o, c_k, c_v)], axis=1))
    down_own = lax.dynamic_slice_in_dim(f_down, rank * unit, unit, axis=0)
    up_own = lax.dynamic_slice_in_dim(
        f_up.reshape(block, n_dp, n_sp, unit), rank, 1, axis=2
    ).reshape(block, n_dp * unit)
    third = from_dp(
        jnp.concatenate([up_own, down_own.reshape(block, unit * width // block)], axis=1)
    )
    up = third[:, : n_dp * unit]
    down = third[:, n_dp * unit :].reshape(n_dp * unit, width)

    qkv_w = first[:, : 3 * own]
    vecs = first[:, 3 * own : 3 * own + 6].astype(F32).T
    ga, ba, gc, bc, gf, bf = (vecs[i : i + 1] for i in range(6))
    o_full, cq_full, co_full = sp_gather(
        n_sp, 2, [second[:, i * own : (i + 1) * own] for i in range(3)], (1, 1, 1)
    )
    cq_own = second[:, own : 2 * own]
    ckv_own = second[:, 3 * own :]

    x, txt, cot = sp_gather(n_sp, 1, [frames[0], text[0], cotangent[0]], (0, 0, 0))
    x = x.astype(F32)

    hat1, _ = norm_parts(x)
    h1 = (hat1 * ga + ba).astype(BF)
    qkv = mm(h1, qkv_w).astype(BF)
    q, k, v = (qkv[:, i * own : (i + 1) * own] for i in range(3))
    ctx_own, lse = attend(q, k, v, flen, True)
    (ctx,) = sp_gather(n_sp, 3, [ctx_own], (1,))
    mid = x + mm(ctx, o_full)
    hat2, inv2 = norm_parts(mid)
    h2 = (hat2 * gc + bc).astype(BF)
    q2 = mm(h2, cq_own).astype(BF)
    kv2 = mm(txt, ckv_own).astype(BF)
    k2, v2 = kv2[:, :own], kv2[:, own:]
    ctx2_own, lse2 = attend(q2, k2, v2, tlen, False)
    (ctx2,) = sp_gather(n_sp, 4, [ctx2_own], (1,))
    after = mid + mm(ctx2, co_full)
    hat3, _ = norm_parts(after)
    h3 = (hat3 * gf + bf).astype(BF)
    u = mm(h3, up)
    act, slope = gelu_parts(u)
    act = act.astype(BF)
    after_own = own_rows(after)
    output = (after_own + sp_scatter(n_sp, 5, mm(act, down))).astype(BF).reshape(frames.shape)

    du = (mm_t(cot, down) * slope).astype(BF)
    part_down = t_mm(act, cot).astype(BF).reshape(n_dp * block, unit * width // block)
    part_ffn = jnp.concatenate([part_down, t_mm(h3, du).astype(BF)], axis=1)
    sum_ffn = lax.psum_scatter(part_ffn, "dp", scatter_dimension=0, tiled=True)
    e3 = sp_scatter(n_sp, 6, mm_t(du, up))
    hat, inv = norm_parts(after_own)
    d_after_own = cotangent[0].astype(F32) + norm_back(e3, hat, inv, gf)
    sums = [jnp.sum(e3 * hat, axis=0), jnp.sum(e3, axis=0)]
    (da2,) = sp_gather(n_sp, 7, [d_after_own.astype(BF)], (0,))
    dctx2 = mm_t(da2, lax.dynamic_slice_in_dim(co_full, rank * own, own, axis=0)).astype(BF)
    dq2, dk2, dv2 = attend_back(q2, k2, v2, dctx2, lse2, tlen, False)
    (dq2_full,) = sp_gather(n_sp, 8, [dq2], (1,))
    part_cross = jnp.concatenate(
        [t_mm(ctx2, own_cols(da2)), t_mm(h2, dq2), t_mm(txt, jnp.concatenate([dk2, dv2], axis=1))],
        axis=1,
    ).astype(BF)
    sum_cross = lax.psum_scatter(part_cross, "dp", scatter_dimension=0, tiled=True)
    grad_text = sp_scatter(n_sp, 9, mm_t(jnp.concatenate([dk2, dv2], axis=1), ckv_own))
    e2 = mm_t(dq2_full, cq_full)
    back2 = norm_back(e2, hat2, inv2, gc)
    da = (da2.astype(F32) + back2).astype(BF)
    e2_own = own_rows(e2)
    hat2_own = own_rows(hat2)
    d_mid_own = d_after_own + own_rows(back2)
    sums = [jnp.sum(e2_own * hat2_own, axis=0), jnp.sum(e2_own, axis=0)] + sums
    dctx = mm_t(da, lax.dynamic_slice_in_dim(o_full, rank * own, own, axis=0)).astype(BF)
    dq, dk, dv = attend_back(q, k, v, dctx, lse, flen, True)
    dqkv = jnp.concatenate([dq, dk, dv], axis=1)
    e1 = sp_scatter(n_sp, 10, mm_t(dqkv, qkv_w))
    hat, inv = norm_parts(frames[0].astype(F32))
    grad_frames = (d_mid_own + norm_back(e1, hat, inv, ga)).reshape(frames.shape)
    sums = [jnp.sum(e1 * hat, axis=0), jnp.sum(e1, axis=0)] + sums
    sums = jnp.pad(jnp.stack(sums, axis=1), ((0, 0), (0, 122)))
    part_self = jnp.concatenate(
        [t_mm(ctx, own_cols(da)), t_mm(h1, dqkv), sums], axis=1
    ).astype(BF)
    sum_self = lax.psum_scatter(part_self, "dp", scatter_dimension=0, tiled=True)

    (done,) = sp_gather(
        n_sp, 11, [jnp.concatenate([sum_ffn, sum_cross, sum_self], axis=1)], (0,)
    )
    done = done.reshape(n_sp, block, done.shape[1]).astype(F32)
    at = unit * width // block
    grad_down = done[:, :, :at].reshape(n_sp * unit, width)
    grad_up = done[:, :, at : at + n_dp * unit].reshape(n_sp, block, n_dp, unit)
    grad_up = jnp.transpose(grad_up, (1, 2, 0, 3)).reshape(block, hidden)
    at += n_dp * unit
    squares = []
    for _ in range(8):
        squares.append(jnp.transpose(done[:, :, at : at + own], (1, 0, 2)).reshape(block, width))
        at += own
    g_co, g_cq, g_ck, g_cv, g_o, g_q, g_k, g_v = squares
    vec = jnp.sum(done[:, :, at : at + 6], axis=0)
    return (
        output, grad_frames, grad_text.reshape(text.shape),
        g_q, g_k, g_v, g_o, g_cq, g_ck, g_cv, g_co, grad_up, grad_down,
    ) + tuple(vec[:, i] for i in range(6))


def solution(mesh):
    rows, flat, vec = P("dp", "sp", None), P("dp", None), P("dp")
    return jax.shard_map(
        partial(on_device, mesh.shape["dp"], mesh.shape["sp"]),
        mesh=mesh,
        in_specs=(rows, rows, vec, vec, rows) + (flat,) * 10 + (vec,) * 6,
        out_specs=(rows, rows, rows) + (flat,) * 10 + (vec,) * 6,
        check_vma=False,
    )
```

```python
from functools import partial

import jax
import jax.numpy as jnp
from jax import lax
from jax.experimental import pallas as pl
from jax.experimental.pallas import tpu as pltpu
from jax.sharding import PartitionSpec as P

HEAD_DIM = 64
EPS = 1e-05
NEGATIVE = -1e30
BF = jnp.bfloat16
F32 = jnp.float32


def mm(a, b):
    return jnp.dot(a, b, preferred_element_type=F32)


def mm_t(a, b):
    return lax.dot_general(a, b, (((1,), (1,)), ((), ())), preferred_element_type=F32)


def t_mm(a, b):
    return lax.dot_general(a, b, (((0,), (0,)), ((), ())), preferred_element_type=F32)


def norm_parts(rows):
    centre = jnp.mean(rows, axis=-1, keepdims=True)
    spread = jnp.mean(jnp.square(rows - centre), axis=-1, keepdims=True)
    inv = lax.rsqrt(spread + EPS)
    return (rows - centre) * inv, inv


def norm_back(grad, xhat, inv, gain):
    scaled = grad * gain
    return inv * (
        scaled
        - jnp.mean(scaled, axis=-1, keepdims=True)
        - xhat * jnp.mean(scaled * xhat, axis=-1, keepdims=True)
    )


def dot_nt(a, b):
    return lax.dot_general(a, b, (((1,), (1,)), ((), ())), preferred_element_type=F32)


def key_bias(length, n_keys, n_queries, causal):
    rows = lax.broadcasted_iota(jnp.int32, (n_keys, 1), 0)
    bias = jnp.where(rows < length, 0.0, NEGATIVE)
    if not causal:
        return bias, None
    key = lax.broadcasted_iota(jnp.int32, (n_queries, n_queries), 0)
    query = lax.broadcasted_iota(jnp.int32, (n_queries, n_queries), 1)
    return bias, jnp.where(key <= query, 0.0, NEGATIVE)


def scores_t(keys, queries, bias, corner):
    scores = dot_nt(keys, queries)
    if corner is None:
        return scores + bias
    n = corner.shape[0]
    low = scores[-n:] + (bias[-n:] + corner)
    if keys.shape[0] == n:
        return low
    return jnp.concatenate([scores[:-n] + bias[:-n], low], axis=0)


def attend_kernel(causal, step, length_ref, q_ref, k_ref, v_ref, ctx_ref, lse_ref, vt, ctxt):
    heads = q_ref.shape[1] // HEAD_DIM
    n_rows, n_keys = q_ref.shape[0], k_ref.shape[0]
    vt[...] = v_ref[...].T
    lane = lax.broadcasted_iota(jnp.int32, (1, q_ref.shape[1]), 1) // HEAD_DIM
    bias, corner = key_bias(length_ref[0], n_keys, step, causal)

    def one_head(head, carry):
        mask = jnp.where(lane == head, HEAD_DIM**-0.5, 0.0).astype(BF)
        dims = pl.ds(pl.multiple_of(head * HEAD_DIM, HEAD_DIM), HEAD_DIM)
        for at in range(0, n_rows, step):
            seen = at + step if causal else n_keys
            queries = q_ref[at : at + step, :] * mask
            scores = scores_t(k_ref[:seen, :], queries, bias[:seen], corner)
            top = jnp.max(scores, axis=0, keepdims=True)
            raised = jnp.exp(scores - top)
            total = jnp.sum(raised, axis=0, keepdims=True)
            mixed = jnp.dot(vt[dims, :seen], raised.astype(BF), preferred_element_type=F32)
            ctxt[dims, at : at + step] = mixed / total
            lse_ref[pl.ds(head, 1), at : at + step] = top + jnp.log(total)
        return carry

    lax.fori_loop(0, heads, one_head, 0)
    ctx_ref[...] = ctxt[...].T.astype(BF)


def attend_back_kernel(
    causal, step, length_ref, q_ref, k_ref, v_ref, d_ref, lse_ref, dq_ref, dk_ref, dv_ref,
    kt, dqt, dk_sum, dv_sum,
):
    heads = q_ref.shape[1] // HEAD_DIM
    n_rows, n_keys = q_ref.shape[0], k_ref.shape[0]
    kt[...] = k_ref[...].T
    dk_sum[...] = jnp.zeros_like(dk_sum)
    dv_sum[...] = jnp.zeros_like(dv_sum)
    lane = lax.broadcasted_iota(jnp.int32, (1, q_ref.shape[1]), 1) // HEAD_DIM
    bias, corner = key_bias(length_ref[0], n_keys, step, causal)

    def one_head(head, carry):
        mask = jnp.where(lane == head, HEAD_DIM**-0.5, 0.0).astype(BF)
        plain = jnp.where(lane == head, 1.0, 0.0).astype(BF)
        dims = pl.ds(pl.multiple_of(head * HEAD_DIM, HEAD_DIM), HEAD_DIM)
        for at in range(0, n_rows, step):
            seen = at + step if causal else n_keys
            queries = q_ref[at : at + step, :] * mask
            grads = d_ref[at : at + step, :] * plain
            scores = scores_t(k_ref[:seen, :], queries, bias[:seen], corner)
            probs = jnp.exp(scores - lse_ref[pl.ds(head, 1), at : at + step])
            dprobs = dot_nt(v_ref[:seen, :], grads)
            inner = jnp.sum(probs * dprobs, axis=0, keepdims=True)
            dscores = (probs * (dprobs - inner)).astype(BF)
            dqt[dims, at : at + step] = jnp.dot(
                kt[dims, :seen], dscores, preferred_element_type=F32
            ) * (HEAD_DIM**-0.5)
            dk_sum[:seen, :] += jnp.dot(dscores, queries, preferred_element_type=F32)
            dv_sum[:seen, :] += jnp.dot(probs.astype(BF), grads, preferred_element_type=F32)
        return carry

    lax.fori_loop(0, heads, one_head, 0)
    dq_ref[...] = dqt[...].T.astype(BF)
    dk_ref[...] = dk_sum[...].astype(BF)
    dv_ref[...] = dv_sum[...].astype(BF)


STEP = 256
VMEM = pl.BlockSpec(memory_space=pltpu.VMEM)
SMEM = pl.BlockSpec(memory_space=pltpu.SMEM)
LIMIT = 60 * 2**20


def lse_rows(q):
    return max(8, q.shape[1] // HEAD_DIM)


def attend(q, k, v, length, causal):
    n_rows, own = q.shape
    n_keys = k.shape[0]
    work = n_rows * n_keys * own
    return pl.pallas_call(
        partial(attend_kernel, causal, STEP),
        out_shape=(
            jax.ShapeDtypeStruct((n_rows, own), BF),
            jax.ShapeDtypeStruct((lse_rows(q), n_rows), F32),
        ),
        in_specs=[SMEM, VMEM, VMEM, VMEM],
        out_specs=(VMEM, VMEM),
        scratch_shapes=[pltpu.VMEM((own, n_keys), BF), pltpu.VMEM((own, n_rows), F32)],
        compiler_params=pltpu.CompilerParams(vmem_limit_bytes=LIMIT),
        cost_estimate=pl.CostEstimate(
            flops=8 * work, bytes_accessed=4 * q.size * 2, transcendentals=work // HEAD_DIM
        ),
        name="attend",
    )(length, q, k, v)


def attend_back(q, k, v, dctx, lse, length, causal):
    n_rows, own = q.shape
    n_keys = k.shape[0]
    work = n_rows * n_keys * own
    return pl.pallas_call(
        partial(attend_back_kernel, causal, STEP),
        out_shape=(
            jax.ShapeDtypeStruct((n_rows, own), BF),
            jax.ShapeDtypeStruct((n_keys, own), BF),
            jax.ShapeDtypeStruct((n_keys, own), BF),
        ),
        in_specs=[SMEM] + [VMEM] * 5,
        out_specs=(VMEM, VMEM, VMEM),
        scratch_shapes=[
            pltpu.VMEM((own, n_keys), BF),
            pltpu.VMEM((own, n_rows), F32),
            pltpu.VMEM((n_keys, own), F32),
            pltpu.VMEM((n_keys, own), F32),
        ],
        compiler_params=pltpu.CompilerParams(vmem_limit_bytes=LIMIT),
        cost_estimate=pl.CostEstimate(
            flops=20 * work, bytes_accessed=7 * q.size * 2, transcendentals=work // HEAD_DIM
        ),
        name="attend_back",
    )(length, q, k, v, dctx, lse)


def sp_place(n_sp):
    me = lax.axis_index("sp")
    side = lax.rem(me, 2)
    return me, me // 2, side, me + 1 - 2 * side, n_sp // 2


def sp_barrier(n_sp):
    me, y, side, partner, n_y = sp_place(n_sp)
    barrier = pltpu.get_barrier_semaphore()
    pl.semaphore_signal(barrier, inc=1, device_id={"sp": partner})
    for far in range(1, n_y):
        peer = lax.rem(y + far, n_y) * 2 + side
        pl.semaphore_signal(barrier, inc=1, device_id={"sp": peer})
    pl.semaphore_wait(barrier, n_y)


def remote(src, dst, send, recv, peer):
    return pltpu.make_async_remote_copy(
        src_ref=src, dst_ref=dst, send_sem=send, recv_sem=recv, device_id={"sp": peer}
    )


def gather_kernel(n_sp, axes, *refs):
    count = len(axes)
    ins, outs = refs[:count], refs[count : 2 * count]
    send, recv = refs[2 * count :]
    me, y, side, partner, n_y = sp_place(n_sp)

    def spot(which, owner):
        size = ins[which].shape[axes[which]]
        span = pl.ds(pl.multiple_of(owner * size, size), size)
        return outs[which].at[span] if axes[which] == 0 else outs[which].at[:, span]

    sp_barrier(n_sp)
    copies = []
    for which in range(count):
        for far in range(1, n_y):
            peer = lax.rem(y + far, n_y) * 2 + side
            copies.append(
                remote(ins[which], spot(which, me), send.at[which, far], recv.at[which, far], peer)
            )
            copies[-1].start()
        copies.append(
            remote(ins[which], spot(which, me), send.at[which, 0], recv.at[which, 0], partner)
        )
        copies[-1].start()
    for which in range(count):
        spot(which, me)[...] = ins[which][...]
    relays = []
    for which in range(count):
        for far in range(1, n_y):
            copies[which * n_y + far - 1].wait_recv()
            origin = lax.rem(y + n_y - far, n_y) * 2 + side
            at = spot(which, origin)
            slot = n_y - 1 + far
            relays.append(remote(at, at, send.at[which, slot], recv.at[which, slot], partner))
            relays[-1].start()
    for which in range(count):
        for far in range(1, n_y):
            copies[which * n_y + far - 1].wait_send()
        copies[which * n_y + n_y - 1].wait()
    for copy in relays:
        copy.wait()


def sp_gather(n_sp, ident, blocks, axes):
    shapes = []
    for block, axis in zip(blocks, axes):
        shape = list(block.shape)
        shape[axis] *= n_sp
        shapes.append(jax.ShapeDtypeStruct(tuple(shape), block.dtype))
    sent = sum(block.size * block.dtype.itemsize for block in blocks) * n_sp
    return pl.pallas_call(
        partial(gather_kernel, n_sp, axes),
        out_shape=tuple(shapes),
        in_specs=[VMEM] * len(blocks),
        out_specs=(VMEM,) * len(blocks),
        scratch_shapes=[
            pltpu.SemaphoreType.DMA((len(blocks), n_sp)),
            pltpu.SemaphoreType.DMA((len(blocks), n_sp)),
        ],
        compiler_params=pltpu.CompilerParams(
            collective_id=ident, has_side_effects=True, vmem_limit_bytes=LIMIT
        ),
        cost_estimate=pl.CostEstimate(flops=0, bytes_accessed=20 * sent, transcendentals=0),
        name="sp_gather",
    )(*blocks)


def scatter_kernel(n_sp, count, *refs):
    parts, outs = refs[:count], refs[count : 2 * count]
    nears, chips, fars = (refs[at * count : (at + 1) * count] for at in (2, 3, 4))
    send, recv = refs[5 * count :]
    me, y, side, partner, n_y = sp_place(n_sp)

    def mine(which, owner):
        size = outs[which].shape[0]
        return parts[which].at[pl.ds(pl.multiple_of(owner * size, size), size)]

    sp_barrier(n_sp)
    firsts, seconds = {}, {}
    for which in range(count):
        for far in range(1, n_y + 1):
            row = lax.rem(y + far, n_y)
            slot = far % n_y
            firsts[which, slot] = remote(
                mine(which, row * 2 + 1 - side), nears[which].at[slot],
                send.at[which, slot], recv.at[which, slot], partner,
            )
            firsts[which, slot].start()
    for which in range(count):
        for far in range(1, n_y):
            peer = lax.rem(y + far, n_y) * 2 + side
            firsts[which, far].wait_recv()
            chips[which][far] = (
                mine(which, peer)[...].astype(F32) + nears[which][far].astype(F32)
            ).astype(BF)
            slot = n_y - 1 + far
            seconds[which, far] = remote(
                chips[which].at[far], fars[which].at[far],
                send.at[which, slot], recv.at[which, slot], peer,
            )
            seconds[which, far].start()
    for which in range(count):
        firsts[which, 0].wait_recv()
        outs[which][...] = mine(which, me)[...].astype(F32) + nears[which][0].astype(F32)
        for far in range(1, n_y):
            seconds[which, far].wait_recv()
            outs[which][...] += fars[which][far].astype(F32)
    for copy in list(firsts.values()) + list(seconds.values()):
        copy.wait_send()


def sp_scatter(n_sp, ident, parts):
    n_y = n_sp // 2
    shapes = [(part.shape[0] // n_sp, part.shape[1]) for part in parts]
    rooms = [pltpu.VMEM((n_y,) + shape, BF) for shape in shapes]
    sent = sum(part.size for part in parts)
    return pl.pallas_call(
        partial(scatter_kernel, n_sp, len(parts)),
        out_shape=tuple(jax.ShapeDtypeStruct(shape, F32) for shape in shapes),
        in_specs=[VMEM] * len(parts),
        out_specs=(VMEM,) * len(parts),
        scratch_shapes=rooms * 3 + [pltpu.SemaphoreType.DMA((len(parts), n_sp))] * 2,
        compiler_params=pltpu.CompilerParams(
            collective_id=ident, has_side_effects=True, vmem_limit_bytes=LIMIT
        ),
        cost_estimate=pl.CostEstimate(flops=0, bytes_accessed=40 * sent, transcendentals=0),
        name="sp_scatter",
    )(*(part.astype(BF) for part in parts))


def dp_sum_kernel(n_dp, in_ref, out_ref, land, send, recv):
    me = lax.axis_index("dp")
    barrier = pltpu.get_barrier_semaphore()
    peers = [lax.rem(me + far, n_dp) for far in range(n_dp)]
    for peer in peers[1:]:
        pl.semaphore_signal(barrier, inc=1, device_id={"dp": peer})
    pl.semaphore_wait(barrier, n_dp - 1)
    copies = []
    for far in range(1, n_dp):
        copies.append(
            pltpu.make_async_remote_copy(
                src_ref=in_ref.at[peers[far]], dst_ref=land.at[far],
                send_sem=send.at[far], recv_sem=recv.at[far], device_id={"dp": peers[far]},
            )
        )
        copies[-1].start()
    out_ref[...] = in_ref[me].astype(F32)
    for far in range(1, n_dp):
        copies[far - 1].wait_recv()
        out_ref[...] += land[far].astype(F32)
    for copy in copies:
        copy.wait_send()


def dp_sum(ident, blocks):
    n_dp = blocks.shape[0]
    return pl.pallas_call(
        partial(dp_sum_kernel, n_dp),
        out_shape=jax.ShapeDtypeStruct(blocks.shape[1:], F32),
        in_specs=[VMEM],
        out_specs=VMEM,
        scratch_shapes=[
            pltpu.VMEM(blocks.shape, blocks.dtype),
            pltpu.SemaphoreType.DMA((n_dp,)),
            pltpu.SemaphoreType.DMA((n_dp,)),
        ],
        compiler_params=pltpu.CompilerParams(
            collective_id=ident, has_side_effects=True, vmem_limit_bytes=LIMIT
        ),
        cost_estimate=pl.CostEstimate(flops=0, bytes_accessed=20 * blocks.size, transcendentals=0),
        name="dp_sum",
    )(blocks)


def gelu_parts(u):
    phi = 0.5 * (1.0 + lax.erf(u * (2.0**-0.5)))
    slope = phi + u * jnp.exp(-0.5 * u * u) * ((2.0 * jnp.pi) ** -0.5)
    return u * phi, slope


def on_device(n_dp, n_sp, *arrays):
    (
        frames, text, frame_len, text_len, cotangent,
        w_q, w_k, w_v, w_o, c_q, c_k, c_v, c_o, f_up, f_down,
        gain_a, bias_a, gain_c, bias_c, gain_f, bias_f,
    ) = arrays
    clips, local, width = frames.shape
    assert clips == 1
    rank = lax.axis_index("sp")
    own = width // n_sp
    block = w_q.shape[0]
    hidden = f_up.shape[1]
    unit = f_down.shape[0] // n_sp
    flen, tlen = frame_len, text_len

    def own_cols(weight):
        return lax.dynamic_slice_in_dim(weight, rank * own, own, axis=1)

    def own_rows(rows):
        return lax.dynamic_slice_in_dim(rows, rank * local, local, axis=0)

    def from_dp(part):
        return lax.all_gather(part, "dp", axis=0, tiled=True)

    small = jnp.stack([gain_a, bias_a, gain_c, bias_c, gain_f, bias_f], axis=1)
    small = jnp.pad(small, ((0, 0), (0, 128 - small.shape[1])))
    first = from_dp(jnp.concatenate([own_cols(w) for w in (w_q, w_k, w_v)] + [small], axis=1))
    second = from_dp(jnp.concatenate([own_cols(w) for w in (w_o, c_q, c_o, c_k, c_v)], axis=1))
    down_own = lax.dynamic_slice_in_dim(f_down, rank * unit, unit, axis=0)
    up_own = lax.dynamic_slice_in_dim(
        f_up.reshape(block, n_dp, n_sp, unit), rank, 1, axis=2
    ).reshape(block, n_dp * unit)
    third = from_dp(
        jnp.concatenate([up_own, down_own.reshape(block, unit * width // block)], axis=1)
    )
    up = third[:, : n_dp * unit]
    down = third[:, n_dp * unit :].reshape(n_dp * unit, width)

    qkv_w = first[:, : 3 * own]
    vecs = first[:, 3 * own : 3 * own + 6].astype(F32).T
    ga, ba, gc, bc, gf, bf = (vecs[i : i + 1] for i in range(6))
    o_full, cq_full, co_full = sp_gather(
        n_sp, 2, [second[:, i * own : (i + 1) * own] for i in range(3)], (1, 1, 1)
    )
    cq_own = second[:, own : 2 * own]
    ckv_own = second[:, 3 * own :]

    x, txt, cot = sp_gather(n_sp, 1, [frames[0], text[0], cotangent[0]], (0, 0, 0))
    x = x.astype(F32)

    hat1, _ = norm_parts(x)
    h1 = (hat1 * ga + ba).astype(BF)
    qkv = mm(h1, qkv_w).astype(BF)
    q, k, v = (qkv[:, i * own : (i + 1) * own] for i in range(3))
    ctx_own, lse = attend(q, k, v, flen, True)
    (ctx,) = sp_gather(n_sp, 3, [ctx_own], (1,))
    mid = x + mm(ctx, o_full)
    hat2, inv2 = norm_parts(mid)
    h2 = (hat2 * gc + bc).astype(BF)
    q2 = mm(h2, cq_own).astype(BF)
    kv2 = mm(txt, ckv_own).astype(BF)
    k2, v2 = kv2[:, :own], kv2[:, own:]
    ctx2_own, lse2 = attend(q2, k2, v2, tlen, False)
    (ctx2,) = sp_gather(n_sp, 4, [ctx2_own], (1,))
    after = mid + mm(ctx2, co_full)
    hat3, _ = norm_parts(after)
    h3 = (hat3 * gf + bf).astype(BF)
    u = mm(h3, up)
    act, slope = gelu_parts(u)
    act = act.astype(BF)
    after_own = own_rows(after)
    output = lax.psum_scatter(
        mm(act, down).astype(BF), "sp", scatter_dimension=0, tiled=True
    ).astype(F32)
    output = (after_own + output).astype(BF).reshape(frames.shape)

    du = (mm_t(cot, down) * slope).astype(BF)
    part_down = t_mm(act, cot).astype(BF).reshape(n_dp * block, unit * width // block)
    part_ffn = jnp.concatenate([part_down, t_mm(h3, du).astype(BF)], axis=1)
    part_ffn, du = lax.optimization_barrier((part_ffn, du))
    sum_ffn = lax.psum_scatter(part_ffn, "dp", scatter_dimension=0, tiled=True)
    (e3,) = sp_scatter(n_sp, 6, [mm_t(du, up)])
    hat, inv = norm_parts(after_own)
    d_after_own = cotangent[0].astype(F32) + norm_back(e3, hat, inv, gf)
    sums = [jnp.sum(e3 * hat, axis=0), jnp.sum(e3, axis=0)]
    (da2,) = sp_gather(n_sp, 7, [d_after_own.astype(BF)], (0,))
    dctx2 = mm_t(da2, lax.dynamic_slice_in_dim(co_full, rank * own, own, axis=0)).astype(BF)
    dq2, dk2, dv2 = attend_back(q2, k2, v2, dctx2, lse2, tlen, False)
    dkv2 = jnp.concatenate([dk2, dv2], axis=1)
    part_cross = jnp.concatenate(
        [t_mm(ctx2, own_cols(da2)), t_mm(h2, dq2), t_mm(txt, dkv2)], axis=1
    ).astype(BF)
    part_cross, dq2 = lax.optimization_barrier((part_cross, dq2))
    sum_cross = lax.psum_scatter(part_cross, "dp", scatter_dimension=0, tiled=True)
    (dq2_full,) = sp_gather(n_sp, 8, [dq2], (1,))
    e2 = mm_t(dq2_full, cq_full)
    back2 = norm_back(e2, hat2, inv2, gc)
    da = (da2.astype(F32) + back2).astype(BF)
    e2_own = own_rows(e2)
    hat2_own = own_rows(hat2)
    d_mid_own = d_after_own + own_rows(back2)
    sums = [jnp.sum(e2_own * hat2_own, axis=0), jnp.sum(e2_own, axis=0)] + sums
    dctx = mm_t(da, lax.dynamic_slice_in_dim(o_full, rank * own, own, axis=0)).astype(BF)
    dq, dk, dv = attend_back(q, k, v, dctx, lse, flen, True)
    dqkv = jnp.concatenate([dq, dk, dv], axis=1)
    part_self = jnp.concatenate([t_mm(ctx, own_cols(da)), t_mm(h1, dqkv)], axis=1).astype(BF)
    part_self, dqkv = lax.optimization_barrier((part_self, dqkv))
    sum_self = lax.psum_scatter(part_self, "dp", scatter_dimension=0, tiled=True)
    e1, grad_text = sp_scatter(n_sp, 10, [mm_t(dqkv, qkv_w), mm_t(dkv2, ckv_own)])
    hat, inv = norm_parts(frames[0].astype(F32))
    grad_frames = (d_mid_own + norm_back(e1, hat, inv, ga)).reshape(frames.shape)
    sums = [jnp.sum(e1 * hat, axis=0), jnp.sum(e1, axis=0)] + sums
    sums = jnp.transpose(jnp.stack(sums).reshape(6, n_dp, block), (1, 0, 2))
    sums = jnp.pad(sums, ((0, 0), (0, 2), (0, 128 - block)))
    vec = dp_sum(12, sums)
    sum_ffn, sum_cross, vec = lax.optimization_barrier((sum_ffn, sum_cross, vec))
    done, = sp_gather(n_sp, 11, [jnp.concatenate([sum_ffn, sum_cross], axis=1)], (0,))
    last, vec = sp_gather(n_sp, 13, [sum_self, vec], (0, 0))
    done = done.reshape(n_sp, block, done.shape[1]).astype(F32)
    last = last.reshape(n_sp, block, last.shape[1]).astype(F32)
    vec = jnp.sum(vec.reshape(n_sp, 8, 128), axis=0)[:6, :block]
    at = unit * width // block
    grad_down = done[:, :, :at].reshape(n_sp * unit, width)
    grad_up = done[:, :, at : at + n_dp * unit].reshape(n_sp, block, n_dp, unit)
    grad_up = jnp.transpose(grad_up, (1, 2, 0, 3)).reshape(block, hidden)
    at += n_dp * unit

    def square(rows, at):
        return jnp.transpose(rows[:, :, at : at + own], (1, 0, 2)).reshape(block, width)

    g_co, g_cq, g_ck, g_cv = (square(done, at + i * own) for i in range(4))
    g_o, g_q, g_k, g_v = (square(last, i * own) for i in range(4))
    return (
        output, grad_frames, grad_text.reshape(text.shape),
        g_q, g_k, g_v, g_o, g_cq, g_ck, g_cv, g_co, grad_up, grad_down,
    ) + tuple(vec[i] for i in range(6))


def solution(mesh):
    rows, flat, vec = P("dp", "sp", None), P("dp", None), P("dp")
    return jax.shard_map(
        partial(on_device, mesh.shape["dp"], mesh.shape["sp"]),
        mesh=mesh,
        in_specs=(rows, rows, vec, vec, rows) + (flat,) * 10 + (vec,) * 6,
        out_specs=(rows, rows, rows) + (flat,) * 10 + (vec,) * 6,
        check_vma=False,
    )
```
